128 devices in a mesh: row: 16 (over z, x), col: 8 (over y, core).
Axes of the slice: x: 4, y: 4, z: 4, core: 2. Of those that a mesh axis runs over, the one named last changes fastest.
Arguments:
- tokens: bfloat16 [1024, 12288], P('col', 'row'), may hold values from -16 to 16
- norm_gain: float32 [12288], P('row'), may hold values from 0.25 to 1.75
- weight_in: bfloat16 [12288, 49152], P('row', 'col'), may hold values from -0.0546875 to 0.0546875
- weight_out: bfloat16 [49152, 12288], P('col', 'row'), may hold values from -0.02734375 to 0.02734375
Outputs:
- mixed: bfloat16 [1024, 12288], P('col', 'row')
The draws below stay inside these ranges and needn't reach their ends.
All inputs are finite; a program needn't handle non-finite values.
Results may differ from the reference program's by a relative error of at most 0.0051.
Values may be sent and summed in bfloat16 or wider, within the bound.
A program may use at most 128 MiB of HBM per device.

```python
import math
import jax
import jax.numpy as jnp
from jax import lax

D = 12288
FF = 49152
TOKENS = 1024


def draw_tokens(key, part):
    base_key = jax.random.fold_in(key, 17)
    noise_key, col_key, row_key = jax.random.split(base_key, 3)
    position = jnp.arange(D, dtype=jnp.float32) / D
    col_scale = jnp.exp(math.log(3.0) * position + jax.random.uniform(col_key, (D,), jnp.float32, 0.0, math.log(3.0))) / 3.0
    row_scale = jnp.exp(jax.random.uniform(row_key, (TOKENS, 1), jnp.float32, math.log(0.1), 0.0))
    values = jax.random.normal(noise_key, (TOKENS, D), jnp.float32)
    return jnp.clip(values * row_scale * col_scale[None, :], -16.0, 16.0).astype(jnp.bfloat16)


def block_levels(rng, dims, pieces, smallest, largest):
    factor_of, own = 1.0, jax.random.fold_in(rng, 6)
    for dim, blocks in pieces:
        heights = jnp.exp(jax.random.uniform(jax.random.fold_in(own, dim), (blocks,), jnp.float32, smallest / len(pieces), largest / len(pieces)))
        factor_of = factor_of * jnp.repeat(heights, dims[dim] // blocks).reshape([-1 if axis == dim else 1 for axis in range(len(dims))])
    return factor_of


def centred(rng, dims, deviation, limit, cuts=(), held_as=jnp.bfloat16):
    factor_of = block_levels(rng, dims, cuts, -0.22, 0.18) if cuts else 1.0
    result = jax.random.normal(rng, dims, jnp.float32) * deviation * factor_of
    return jnp.minimum(jnp.maximum(result, -limit), limit).astype(held_as)


def setup_inputs(seed: int = 0) -> dict:
    key_of = jax.random.split(jax.random.key(seed), 5)
    tokens = draw_tokens(jax.random.fold_in(key_of[4], 71), 0)
    norm_gain = jnp.clip(1.0 + 0.15 * jax.random.normal(key_of[1], (D,), jnp.float32), 0.25, 1.75)
    weight_in = centred(key_of[2], (D, FF), D ** -0.5, 0.0546875, ((0, 16), (1, 8)))
    weight_out = centred(key_of[3], (FF, D), FF ** -0.5, 0.02734375, ((0, 8), (1, 16)))
    return {"tokens": tokens, "norm_gain": norm_gain, "weight_in": weight_in, "weight_out": weight_out}


epsilon = 1e-05

def reference(tokens, norm_gain, weight_in, weight_out):
    wide_input = tokens.astype(jnp.float32)
    scaled = (wide_input * norm_gain.astype(jnp.float32)[None, :]).astype(jnp.bfloat16)
    squares = lax.optimization_barrier(jnp.sum(wide_input * wide_input, axis=1))
    inverse = lax.rsqrt(squares / D + epsilon)
    hidden = jnp.dot(scaled, weight_in, preferred_element_type=jnp.float32) * inverse[:, None]
    active = jax.nn.gelu(hidden, approximate=True).astype(jnp.bfloat16)
    branch = jnp.dot(active, weight_out, preferred_element_type=jnp.float32)
    return (wide_input + branch).astype(jnp.bfloat16)
```

```python
import functools

import jax
import jax.numpy as jnp
from jax import lax
from jax.experimental import pallas as pl
from jax.experimental.pallas import tpu as pltpu
from jax.sharding import PartitionSpec as P

D = 12288
EPSILON = 1e-05
MESH = pl.DeviceIdType.MESH
F32, BF16 = jnp.float32, jnp.bfloat16

WAVES = 4
LANES = 8
NARROW = 768
BLOCK = 16
TILE = 256


def gelu(v):
    return 0.5 * v * (1.0 + jnp.tanh(0.7978845608028654 * (v + 0.044715 * (v * v * v))))


def kernel(
    tokens_ref, gain_ref, w1_hbm, w2_hbm, out_ref,
    w1, w2, raw, scaled, rs1, rs2, total, active, branch, own, out_send, out_recv, squares, inverse,
    w1_sem, w2_sem, tok_ssem, tok_rsem, out_ssem, out_rsem, sq_ssem, sq_rsem, ring_ssem, ring_rsem,
):
    row, col = lax.axis_index("row"), lax.axis_index("col")
    x, z = lax.rem(row, 4), lax.div(row, 4)

    def w1_copy(s):
        return pltpu.make_async_copy(w1_hbm.at[:, pl.ds(pl.multiple_of(s * NARROW, NARROW), NARROW)], w1.at[s], w1_sem.at[s])

    def w2_copy(s):
        return pltpu.make_async_copy(w2_hbm.at[pl.ds(pl.multiple_of(s * NARROW, NARROW), NARROW)], w2.at[s], w2_sem.at[s])

    for s in range(LANES):
        w1_copy(s).start()
    for s in range(LANES):
        w2_copy(s).start()

    barrier = pltpu.get_barrier_semaphore()
    for i in range(1, 8):
        pl.semaphore_signal(barrier, inc=1, device_id=(row, lax.rem(col + i, 8)), device_id_type=MESH)
    for i in range(1, 16):
        pl.semaphore_signal(barrier, inc=1, device_id=(lax.rem(row + i, 16), col), device_id_type=MESH)
    pl.semaphore_wait(barrier, 22)

    def tok_copy(w, i):
        return pltpu.make_async_remote_copy(
            src_ref=tokens_ref.at[w], dst_ref=raw.at[col, w],
            send_sem=tok_ssem.at[w, i], recv_sem=tok_rsem.at[w, i],
            device_id=(row, lax.rem(col + i, 8)), device_id_type=MESH,
        )

    for w in range(WAVES):
        for i in range(1, 8):
            tok_copy(w, i).start()
    raw[col] = tokens_ref[...]

    def place(s):
        second = lax.rem(s, 2)
        step = 1 - 2 * lax.rem(lax.div(s, 2), 2)
        p = x * (1 - second) + z * second
        q = z * (1 - second) + x * second
        p_next, q_next = lax.rem(p + step + 4, 4), lax.rem(q + step + 4, 4)
        first_row = second * (p_next * 4 + q) + (1 - second) * (q * 4 + p_next)
        second_row = second * (p * 4 + q_next) + (1 - second) * (q_next * 4 + p)
        return p, q, step, first_row, second_row

    def ring_copy(kind, w, s, k, src, dst, target):
        return pltpu.make_async_remote_copy(
            src_ref=src, dst_ref=dst,
            send_sem=ring_ssem.at[kind, s, k], recv_sem=ring_rsem.at[kind, w, s, k],
            device_id=(target, col), device_id_type=MESH,
        )

    def around(v):
        return lax.rem(v + 8, 4)

    def rs1_copy(w, s, k, target):
        return ring_copy(0, w, s, k, rs1.at[w, s, (k + 3) % 4], rs1.at[w, s, k], target)

    def rs2_copy(w, s, k, target):
        return ring_copy(1, w, s, k, rs2.at[w, s, (k + 3) % 4], rs2.at[w, s, k], target)

    def ag2_copy(w, s, k, p, q, step, target):
        block = active.at[w, s, p * 4 + around(q - step * k)]
        return ring_copy(2, w, s, k, block, block, target)

    def ag1_copy(w, s, k, p, step, target):
        chunk = active.at[w, s, pl.ds(around(p - step * k) * 4, 4)]
        return ring_copy(3, w, s, k, chunk, chunk, target)

    def product(w, s, j, t):
        a = scaled[w, pl.ds(j * 4, 4)].reshape(64, NARROW)
        return jnp.dot(a, w1[s, :, t * TILE:(t + 1) * TILE], preferred_element_type=F32).reshape(4, BLOCK, TILE)

    def rs1_event(w, s, k):
        p, q, step, target, _ = place(s)
        j = around(p - step * (k + 1))
        slot = (k + 3) % 4
        if k > 0:
            rs1_copy(w, s, k - 1, target).wait_recv()
        for t in range(NARROW // TILE):
            part = product(w, s, j, t)
            if k > 0:
                part = part + rs1[w, s, slot, :, :, t * TILE:(t + 1) * TILE].astype(F32)
            rs1[w, s, slot, :, :, t * TILE:(t + 1) * TILE] = part.astype(BF16)

        @pl.when(w > 0)
        def _():
            rs1_copy(w, s, k, target).wait_send()

        rs1_copy(w, s, k, target).start()

    def rs2_event(w, s, k):
        p, q, step, before, target = place(s)
        j = around(q - step * (k + 1))
        slot = (k + 3) % 4
        if k == 0:
            rs1_copy(w, s, 2, before).wait_recv()
            for t in range(NARROW // TILE):
                cols = slice(t * TILE, (t + 1) * TILE)
                total[s, :, :, cols] = product(w, s, p, t) + rs1[w, s, 2, :, :, cols].astype(F32)
            rs2[w, s, slot] = total[s, j].astype(BF16)
        else:
            rs2_copy(w, s, k - 1, target).wait_recv()
            rs2[w, s, slot] = (rs2[w, s, slot].astype(F32) + total[s, j]).astype(BF16)

        @pl.when(w > 0)
        def _():
            rs2_copy(w, s, k, target).wait_send()

        rs2_copy(w, s, k, target).start()

    def ag2_event(w, s, k):
        p, q, step, _, target = place(s)
        if k == 0:
            rs2_copy(w, s, 2, target).wait_recv()
            b = p * 4 + q
            c, first = lax.div(b, 2), 32 * w + 16 * lax.rem(b, 2)
            sub = lax.broadcasted_iota(jnp.int32, (8, 128), 0)
            line = jnp.sum(jnp.where(sub == c, inverse[...], 0.0), axis=0, keepdims=True)
            spot = lax.broadcasted_iota(jnp.int32, (BLOCK, 128), 1) == lax.broadcasted_iota(jnp.int32, (BLOCK, 128), 0) + first
            scale = jnp.sum(jnp.where(spot, jnp.broadcast_to(line, (BLOCK, 128)), 0.0), axis=1, keepdims=True)
            hidden = (rs2[w, s, 2].astype(F32) + total[s, q]) * scale
            active[w, s, b] = gelu(hidden).astype(BF16)
        else:
            ag2_copy(w, s, k - 1, p, q, step, target).wait_recv()

        @pl.when(w > 0)
        def _():
            ag2_copy(w, s, k, p, q, step, target).wait_send()

        ag2_copy(w, s, k, p, q, step, target).start()

    def ag1_event(w, s, k):
        p, q, step, target, before = place(s)
        if k == 0:
            ag2_copy(w, s, 2, p, q, step, before).wait_recv()
        else:
            ag1_copy(w, s, k - 1, p, step, target).wait_recv()

        @pl.when(w > 0)
        def _():
            ag1_copy(w, s, k, p, step, target).wait_send()

        ag1_copy(w, s, k, p, step, target).start()

    def out_copy(w, i):
        peer = lax.rem(col + i, 8)
        return pltpu.make_async_remote_copy(
            src_ref=out_send.at[w, peer], dst_ref=out_recv.at[w, col],
            send_sem=out_ssem.at[w, i], recv_sem=out_rsem.at[w, i],
            device_id=(row, peer), device_id_type=MESH,
        )

    def finish(w, s):
        p, q, step, target, _ = place(s)
        ag1_copy(w, s, 2, p, step, target).wait_recv()

        @pl.when(w == 0)
        def _():
            w2_copy(s).wait()

        def tile(t, carry):
            cols = pl.ds(pl.multiple_of(t * TILE, TILE), TILE)
            got = jnp.dot(active[w, s].reshape(256, NARROW), w2[s, :, cols], preferred_element_type=F32)
            branch[:, cols] = jnp.where(s == 0, 0.0, branch[:, cols]) + got
            return carry

        lax.fori_loop(0, 3, tile, 0)

        @pl.when(s == LANES - 1)
        def _():
            out_send[w] = branch[...].reshape(8, 32, NARROW).astype(BF16)
            own[w] = branch[pl.ds(pl.multiple_of(col * 32, 32), 32)]
            for i in range(1, 8):
                out_copy(w, i).start()

    def deliver(w):
        rows = own[w] + tokens_ref[w].astype(F32)
        for i in range(1, 8):
            out_copy(w, i).wait_recv()
            rows = rows + out_recv[w, lax.rem(col + 8 - i, 8)].astype(F32)
        out_ref[w] = rows.astype(BF16)

    def wait_tokens(w):
        for i in range(1, 8):
            tok_copy(w, i).wait_recv()

    def sq_copy(i):
        return pltpu.make_async_remote_copy(
            src_ref=squares.at[row], dst_ref=squares.at[row],
            send_sem=sq_ssem.at[i], recv_sem=sq_rsem.at[i],
            device_id=(lax.rem(row + i, 16), col), device_id_type=MESH,
        )

    def send_squares():
        ones = jnp.ones((8, NARROW), BF16)
        sub = lax.broadcasted_iota(jnp.int32, (8, 128), 0)

        def one(c, tile):
            v = raw[c].reshape(128, NARROW).astype(F32)
            v = v * v
            high = v.astype(BF16)
            low = (v - high.astype(F32)).astype(BF16)
            dims = (((1,), (1,)), ((), ()))
            sums = lax.dot_general(ones, high, dims, preferred_element_type=F32)
            sums = sums + lax.dot_general(ones, low, dims, preferred_element_type=F32)
            return jnp.where(sub == c, sums, tile)

        squares[row] = lax.fori_loop(0, 8, one, jnp.zeros((8, 128), F32))
        for i in range(1, 16):
            sq_copy(i).start()

    def take_squares():
        for i in range(1, 16):
            sq_copy(i).wait_recv()
        inverse[...] = lax.rsqrt(jnp.sum(squares[...], axis=0) / D + EPSILON)

    def scale_wave(w):
        def one(c, carry):
            v = raw[c, w].astype(F32) * gain_ref[...]
            scaled[w, pl.ds(2 * c, 2)] = v.astype(BF16).reshape(2, BLOCK, NARROW)
            return carry

        lax.fori_loop(0, 8, one, 0)

    def slot(t, carry):
        @pl.when(t == 0)
        def _():
            wait_tokens(0)

        @pl.when(t == 1)
        def _():
            for w in range(1, WAVES):
                wait_tokens(w)

        @pl.when(t < WAVES)
        def _():
            scale_wave(t)

        @pl.when(t == 2)
        def _():
            take_squares()

        for k in range(3):
            def lane(s, carry, k=k):
                if k == 0:
                    @pl.when(t >= 4)
                    def _():
                        finish(t - 4, s)

                    @pl.when(t == 0)
                    def _():
                        w1_copy(s).wait()

                @pl.when((t >= 3) & (t < 7))
                def _():
                    ag1_event(t - 3, s, k)

                @pl.when((t >= 2) & (t < 6))
                def _():
                    ag2_event(t - 2, s, k)

                @pl.when((t >= 1) & (t < 5))
                def _():
                    rs2_event(t - 1, s, k)

                @pl.when(t < 4)
                def _():
                    rs1_event(t, s, k)

                return carry

            lax.fori_loop(0, LANES, lane, 0)

            if k == 0:
                @pl.when(t == 1)
                def _():
                    send_squares()

                @pl.when(t >= 5)
                def _():
                    deliver(t - 5)

        return carry

    lax.fori_loop(0, 7, slot, 0)

    def last(s, carry):
        finish(WAVES - 1, s)
        return carry

    lax.fori_loop(0, LANES, last, 0)
    deliver(WAVES - 2)
    deliver(WAVES - 1)

    def leave(s, carry):
        p, q, step, first_row, second_row = place(s)
        w = WAVES - 1
        for k in range(3):
            rs1_copy(w, s, k, first_row).wait_send()
            rs2_copy(w, s, k, second_row).wait_send()
            ag2_copy(w, s, k, p, q, step, second_row).wait_send()
            ag1_copy(w, s, k, p, step, first_row).wait_send()
        return carry

    lax.fori_loop(0, LANES, leave, 0)
    for i in range(1, 8):
        for w in range(WAVES):
            tok_copy(w, i).wait_send()
            out_copy(w, i).wait_send()
    for i in range(1, 16):
        sq_copy(i).wait_send()


def per_device(tokens, norm_gain, weight_in, weight_out):
    vmem = pl.BlockSpec(memory_space=pltpu.VMEM)
    anywhere = pl.BlockSpec(memory_space=pl.ANY)
    dma = pltpu.SemaphoreType.DMA
    out = pl.pallas_call(
        kernel,
        out_shape=jax.ShapeDtypeStruct((WAVES, 32, NARROW), BF16),
        in_specs=[vmem, vmem, anywhere, anywhere],
        out_specs=vmem,
        scratch_shapes=[
            pltpu.VMEM((LANES, 768, NARROW), BF16),
            pltpu.VMEM((LANES, NARROW, 768), BF16),
            pltpu.VMEM((8, WAVES, 32, 768), BF16),
            pltpu.VMEM((WAVES, 16, BLOCK, 768), BF16),
            pltpu.VMEM((WAVES, LANES, 4, 4, BLOCK, NARROW), BF16),
            pltpu.VMEM((WAVES, LANES, 4, BLOCK, NARROW), BF16),
            pltpu.VMEM((LANES, 4, BLOCK, NARROW), F32),
            pltpu.VMEM((WAVES, LANES, 16, BLOCK, NARROW), BF16),
            pltpu.VMEM((256, 768), F32),
            pltpu.VMEM((WAVES, 32, 768), F32),
            pltpu.VMEM((WAVES, 8, 32, 768), BF16),
            pltpu.VMEM((WAVES, 8, 32, 768), BF16),
            pltpu.VMEM((16, 8, 128), F32),
            pltpu.VMEM((8, 128), F32),
            dma((LANES,)), dma((LANES,)),
            dma((WAVES, 8)), dma((WAVES, 8)),
            dma((WAVES, 8)), dma((WAVES, 8)),
            dma((16,)), dma((16,)),
            dma((4, LANES, 3)), dma((4, WAVES, LANES, 3)),
        ],
        compiler_params=pltpu.CompilerParams(
            collective_id=0, has_side_effects=True, vmem_limit_bytes=67043328
        ),
        name="ffn",
    )(tokens.reshape(WAVES, 32, 768), norm_gain.reshape(1, 768), weight_in, weight_out)
    return out.reshape(128, 768)


def solution(mesh):
    in_specs = (P("col", "row"), P("row"), P("row", "col"), P("col", "row"))
    out_specs = P("col", "row")
    return jax.shard_map(
        per_device, mesh=mesh, in_specs=in_specs, out_specs=out_specs, check_vma=False
    )
```

```python
import functools

import jax
import jax.numpy as jnp
from jax import lax
from jax.experimental import pallas as pl
from jax.experimental.pallas import tpu as pltpu
from jax.sharding import PartitionSpec as P

D = 12288
EPSILON = 1e-05
MESH = pl.DeviceIdType.MESH
F32, BF16 = jnp.float32, jnp.bfloat16

WAVES = 4
LANES = 8
NARROW = 768
BLOCK = 16
TILE = 256
FAR_FIRST = (4, 3, 5, 2, 6, 1, 7)


def gelu(v):
    return 0.5 * v * (1.0 + jnp.tanh(0.7978845608028654 * (v + 0.044715 * (v * v * v))))


def kernel(
    tokens_hbm, gain_hbm, w1_hbm, w2_hbm, out_ref,
    tokens_ref, gain_ref, w1, w2, raw, scaled, part, rs1, rs2, total, active, branch, own, out_send, out_recv, squares, inverse,
    in_sem, w1_sem, w2_sem, tok_ssem, tok_rsem, pair_rsem, out_ssem, out_rsem, sq_ssem, sq_rsem, ring_ssem, ring_rsem,
):
    row, col = lax.axis_index("row"), lax.axis_index("col")
    x, z = lax.rem(row, 4), lax.div(row, 4)

    def w1_copy(s):
        return pltpu.make_async_copy(w1_hbm.at[:, pl.ds(pl.multiple_of(s * NARROW, NARROW), NARROW)], w1.at[s], w1_sem.at[s])

    def w2_copy(s):
        return pltpu.make_async_copy(w2_hbm.at[pl.ds(pl.multiple_of(s * NARROW, NARROW), NARROW)], w2.at[s], w2_sem.at[0])

    inputs = (
        pltpu.make_async_copy(tokens_hbm, tokens_ref, in_sem.at[0]),
        pltpu.make_async_copy(gain_hbm, gain_ref, in_sem.at[1]),
    )
    inputs[0].start()
    barrier = pltpu.get_barrier_semaphore()
    for i in range(1, 8):
        pl.semaphore_signal(barrier, inc=1, device_id=(row, lax.rem(col + i, 8)), device_id_type=MESH)
    for i in range(1, 16):
        pl.semaphore_signal(barrier, inc=1, device_id=(lax.rem(row + i, 16), col), device_id_type=MESH)
    inputs[1].start()
    for s in range(LANES):
        w1_copy(s).start()
    for s in range(LANES):
        w2_copy(s).start()

    inputs[0].wait()
    pl.semaphore_wait(barrier, 22)

    def landed(ref, sem):
        pltpu.make_async_copy(ref, ref, sem).wait()

    partner = col + 1 - 2 * lax.rem(col, 2)

    def tok_copy(w, i):
        return pltpu.make_async_remote_copy(
            src_ref=tokens_ref.at[w], dst_ref=raw.at[col, w], send_sem=tok_ssem.at[0], recv_sem=tok_rsem.at[w],
            device_id=(row, lax.rem(col + 2 * i, 8)), device_id_type=MESH,
        )

    def pair_copy(w, i):
        c = lax.rem(col + 2 * i, 8)
        return pltpu.make_async_remote_copy(
            src_ref=tokens_ref.at[w] if i == 0 else raw.at[c, w], dst_ref=raw.at[c, w],
            send_sem=tok_ssem.at[0], recv_sem=pair_rsem.at[w],
            device_id=(row, partner), device_id_type=MESH,
        )

    for w in range(WAVES):
        for i in (2, 1, 3):
            tok_copy(w, i).start()
        pair_copy(w, 0).start()
    raw[col] = tokens_ref[...]

    def forward_tokens(w):
        landed(raw.at[pl.ds(0, 3), w], tok_rsem.at[w])
        for i in (1, 3, 2):
            pair_copy(w, i).start()

    def wait_tokens(w):
        landed(raw.at[pl.ds(0, 4), w], pair_rsem.at[w])

    def place(s):
        second = lax.rem(s, 2)
        step = 1 - 2 * lax.rem(lax.div(s, 2), 2)
        p = x * (1 - second) + z * second
        q = z * (1 - second) + x * second
        p_next, q_next = lax.rem(p + step + 4, 4), lax.rem(q + step + 4, 4)
        first_row = second * (p_next * 4 + q) + (1 - second) * (q * 4 + p_next)
        second_row = second * (p * 4 + q_next) + (1 - second) * (q_next * 4 + p)
        return p, q, step, first_row, second_row

    def ring_copy(kind, w, s, k, src, dst, target):
        return pltpu.make_async_remote_copy(
            src_ref=src, dst_ref=dst,
            send_sem=ring_ssem.at[kind, s], recv_sem=ring_rsem.at[kind, s, k],
            device_id=(target, col), device_id_type=MESH,
        )

    def around(v):
        return lax.rem(v + 8, 4)

    def rs1_copy(w, s, k, target):
        side = lax.rem(w, 2)
        return ring_copy(0, w, s, k, rs1.at[side, s, (k + 3) % 4], rs1.at[side, s, k], target)

    def rs2_copy(w, s, k, target):
        side = lax.rem(w, 2)
        return ring_copy(1, w, s, k, rs2.at[side, s, (k + 3) % 4], rs2.at[side, s, k], target)

    def ag2_copy(w, s, k, p, q, step, target):
        block = active.at[w, s, p * 4 + around(q - step * k)]
        return ring_copy(2, w, s, k, block, block, target)

    def ag1_copy(w, s, k, p, step, target):
        chunk = active.at[w, s, pl.ds(around(p - step * k) * 4, 4)]
        return ring_copy(3, w, s, k, chunk, chunk, target)

    def own_part(w, s):
        side = lax.rem(w, 2)
        for t in range(NARROW // TILE):
            cols = slice(t * TILE, (t + 1) * TILE)
            got = jnp.dot(scaled[w].reshape(256, 768), w1[s, :, cols], preferred_element_type=F32)
            part[side, s, :, :, cols] = got.reshape(16, BLOCK, TILE)

    def rs1_event(w, s, k):
        p, q, step, target, _ = place(s)
        j = around(p - step * (k + 1))
        side, slot = lax.rem(w, 2), (k + 3) % 4
        mine = part[side, s, pl.ds(j * 4, 4)]
        if k > 0:
            rs1_copy(w, s, k - 1, target).wait_recv()
            mine = mine + rs1[side, s, slot].astype(F32)
        rs1[side, s, slot] = mine.astype(BF16)
        if k > 0:
            rs1_copy(w, s, k - 1, target).wait_send()
        rs1_copy(w, s, k, target).start()

    def rs2_event(w, s, k):
        p, q, step, before, target = place(s)
        j = around(q - step * (k + 1))
        side, slot = lax.rem(w, 2), (k + 3) % 4
        if k == 0:
            rs1_copy(w, s, 2, before).wait_recv()
            total[s] = part[side, s, pl.ds(p * 4, 4)] + rs1[side, s, 2].astype(F32)
            rs1_copy(w, s, 2, before).wait_send()
            rs2[side, s, slot] = total[s, j].astype(BF16)
        else:
            rs2_copy(w, s, k - 1, target).wait_recv()
            rs2[side, s, slot] = (rs2[side, s, slot].astype(F32) + total[s, j]).astype(BF16)
            rs2_copy(w, s, k - 1, target).wait_send()
        rs2_copy(w, s, k, target).start()

    def ag2_event(w, s, k):
        p, q, step, _, target = place(s)
        if k == 0:
            rs2_copy(w, s, 2, target).wait_recv()
            b = p * 4 + q
            c, first = lax.div(b, 2), 32 * w + 16 * lax.rem(b, 2)
            sub = lax.broadcasted_iota(jnp.int32, (8, 128), 0)
            line = jnp.sum(jnp.where(sub == c, inverse[...], 0.0), axis=0, keepdims=True)
            spot = lax.broadcasted_iota(jnp.int32, (BLOCK, 128), 1) == lax.broadcasted_iota(jnp.int32, (BLOCK, 128), 0) + first
            scale = jnp.sum(jnp.where(spot, jnp.broadcast_to(line, (BLOCK, 128)), 0.0), axis=1, keepdims=True)
            hidden = (rs2[lax.rem(w, 2), s, 2].astype(F32) + total[s, q]) * scale
            active[w, s, b] = gelu(hidden).astype(BF16)
            rs2_copy(w, s, 2, target).wait_send()
        else:
            ag2_copy(w, s, k - 1, p, q, step, target).wait_recv()
            ag2_copy(w, s, k - 1, p, q, step, target).wait_send()
        ag2_copy(w, s, k, p, q, step, target).start()

    def ag1_event(w, s, k):
        p, q, step, target, before = place(s)
        if k == 0:
            ag2_copy(w, s, 2, p, q, step, before).wait_recv()
            ag2_copy(w, s, 2, p, q, step, before).wait_send()

            @pl.when(w > 0)
            def _():
                ag1_copy(w, s, 2, p, step, target).wait_send()
        else:
            ag1_copy(w, s, k - 1, p, step, target).wait_recv()
            ag1_copy(w, s, k - 1, p, step, target).wait_send()
        ag1_copy(w, s, k, p, step, target).start()

    def out_copy(w, i):
        peer = lax.rem(col + i, 8)
        return pltpu.make_async_remote_copy(
            src_ref=out_send.at[w, peer], dst_ref=out_recv.at[w, col],
            send_sem=out_ssem.at[0], recv_sem=out_rsem.at[w],
            device_id=(row, peer), device_id_type=MESH,
        )

    def add_chunks(w, s, ks):
        p, q, step, target, _ = place(s)
        side = lax.rem(w, 2)
        if 3 in ks:
            ag1_copy(w, s, 2, p, step, target).wait_recv()
        chunks = [pl.ds(around(p - step * k) * 4, 4) for k in ks]
        a = [active[w, s, chunk].reshape(64, NARROW) for chunk in chunks]
        a = a[0] if len(a) == 1 else jnp.concatenate(a, axis=0)
        for t in range(768 // TILE):
            cols = slice(t * TILE, (t + 1) * TILE)
            got = jnp.dot(a, w2[s, :, cols], preferred_element_type=F32)
            for n, chunk in enumerate(chunks):
                more = got[n * 64:(n + 1) * 64].reshape(4, BLOCK, TILE)
                branch[side, chunk, :, cols] = branch[side, chunk, :, cols] + more

    def send_branch(w):
        side = lax.rem(w, 2)
        out_send[w] = branch[side].reshape(8, 32, 768).astype(BF16)
        own[w] = branch[side, pl.ds(col * 2, 2)].reshape(32, 768)
        for i in FAR_FIRST:
            out_copy(w, i).start()

    def deliver(w):
        rows = own[w] + tokens_ref[w].astype(F32)
        landed(out_recv.at[w, pl.ds(0, 7)], out_rsem.at[w])
        for i in range(1, 8):
            rows = rows + out_recv[w, lax.rem(col + i, 8)].astype(F32)
        out_ref[w] = rows.astype(BF16)

    def sq_copy(i):
        return pltpu.make_async_remote_copy(
            src_ref=squares.at[row], dst_ref=squares.at[row],
            send_sem=sq_ssem.at[0], recv_sem=sq_rsem.at[0],
            device_id=(lax.rem(row + i, 16), col), device_id_type=MESH,
        )

    def square(c):
        v = raw[c].reshape(128, 768).astype(F32)
        v = v * v
        high = v.astype(BF16)
        low = (v - high.astype(F32)).astype(BF16)
        ones, dims = jnp.ones((8, 768), BF16), (((1,), (1,)), ((), ()))
        sums = lax.dot_general(ones, high, dims, preferred_element_type=F32)
        sums = sums + lax.dot_general(ones, low, dims, preferred_element_type=F32)
        squares[row, pl.ds(c, 1)] = sums[:1]

    def take_squares():
        landed(squares.at[pl.ds(0, 15)], sq_rsem.at[0])
        inverse[...] = lax.rsqrt(jnp.sum(squares[...], axis=0) / D + EPSILON)

    def scale_wave(w):
        def one(c, carry):
            v = raw[c, w].astype(F32) * gain_ref[...].reshape(1, 768)
            scaled[w, pl.ds(2 * c, 2)] = v.astype(BF16).reshape(2, BLOCK, NARROW)
            return carry

        lax.fori_loop(0, 8, one, 0)

    inputs[1].wait()
    forward_tokens(0)
    wait_tokens(0)
    scale_wave(0)

    def slot(t, carry):
        for k in range(3):
            if k == 0:
                @pl.when(t == 1)
                def _():
                    wait_tokens(2)
                    wait_tokens(3)

                @pl.when(t == 2)
                def _():
                    take_squares()

                @pl.when(t == 3)
                def _():
                    landed(w2, w2_sem.at[0])

                @pl.when((t >= 3) & (t < 7))
                def _():
                    branch[lax.rem(t + 1, 2)] = jnp.zeros((16, BLOCK, 768), F32)

            if k == 1:
                @pl.when(t == 0)
                def _():
                    forward_tokens(1)

                @pl.when((t >= 1) & (t < 3))
                def _():
                    scale_wave(t + 1)

                @pl.when(t >= 5)
                def _():
                    deliver(t - 5)

            if k == 2:
                @pl.when(t == 0)
                def _():
                    forward_tokens(2)
                    forward_tokens(3)
                    wait_tokens(1)
                    scale_wave(1)

            def lane(s, carry, k=k):
                if k == 0:
                    @pl.when(t == 0)
                    def _():
                        w1_copy(s).wait()
                        own_part(0, s)

                @pl.when((t >= 3) & (t < 7))
                def _():
                    ag1_event(t - 3, s, k)

                @pl.when((t >= 2) & (t < 6))
                def _():
                    ag2_event(t - 2, s, k)

                @pl.when((t >= 1) & (t < 5))
                def _():
                    rs2_event(t - 1, s, k)

                @pl.when(t < 4)
                def _():
                    rs1_event(t, s, k)

                if k == 0:
                    @pl.when(t == 1)
                    def _():
                        square(s)

                    @pl.when(t >= 4)
                    def _():
                        add_chunks(t - 4, s, (2, 3))

                if k == 1:
                    @pl.when((t >= 1) & (t < 3) & (lax.rem(s, 2) == 1))
                    def _():
                        own_part(t + 1, lax.div(s, 2))

                if k == 2:
                    @pl.when((t == 0) | ((t < 3) & (lax.rem(s, 2) == 1)))
                    def _():
                        own_part(t + 1, jnp.where(t == 0, s, 4 + lax.div(s, 2)))

                if k == 1:
                    @pl.when(t >= 3)
                    def _():
                        add_chunks(t - 3, s, (0, 1))

                if k == 2:
                    @pl.when(t == 6)
                    def _():
                        add_chunks(WAVES - 1, s, (2,))

                return carry

            lax.fori_loop(0, LANES, lane, 0)

            if k == 0:
                @pl.when(t == 1)
                def _():
                    for i in range(1, 16):
                        sq_copy(i).start()

                @pl.when(t >= 4)
                def _():
                    send_branch(t - 4)

            if k == 1:
                @pl.when(t == 4)
                def _():
                    landed(raw.at[pl.ds(0, 7)], tok_ssem.at[0])
                    landed(squares.at[pl.ds(0, 15)], sq_ssem.at[0])

            if k == 2:
                @pl.when(t == 6)
                def _():
                    deliver(2)

        return carry

    lax.fori_loop(0, 7, slot, 0)

    def last(s, carry):
        add_chunks(WAVES - 1, s, (3,))
        p, q, step, target, _ = place(s)
        ag1_copy(WAVES - 1, s, 2, p, step, target).wait_send()
        return carry

    lax.fori_loop(0, LANES, last, 0)
    send_branch(WAVES - 1)
    deliver(WAVES - 1)
    landed(out_send.at[:, pl.ds(0, 7)], out_ssem.at[0])


def per_device(tokens, norm_gain, weight_in, weight_out):
    vmem = pl.BlockSpec(memory_space=pltpu.VMEM)
    anywhere = pl.BlockSpec(memory_space=pl.ANY)
    dma = pltpu.SemaphoreType.DMA
    out = pl.pallas_call(
        kernel,
        out_shape=jax.ShapeDtypeStruct((WAVES, 32, NARROW), BF16),
        in_specs=[anywhere] * 4,
        out_specs=vmem,
        scratch_shapes=[
            pltpu.VMEM((WAVES, 32, 768), BF16),
            pltpu.VMEM((768,), F32),
            pltpu.VMEM((LANES, 768, NARROW), BF16),
            pltpu.VMEM((LANES, NARROW, 768), BF16),
            pltpu.VMEM((8, WAVES, 32, 768), BF16),
            pltpu.VMEM((WAVES, 16, BLOCK, 768), BF16),
            pltpu.VMEM((2, LANES, 16, BLOCK, NARROW), F32),
            pltpu.VMEM((2, LANES, 4, 4, BLOCK, NARROW), BF16),
            pltpu.VMEM((2, LANES, 4, BLOCK, NARROW), BF16),
            pltpu.VMEM((LANES, 4, BLOCK, NARROW), F32),
            pltpu.VMEM((WAVES, LANES, 16, BLOCK, NARROW), BF16),
            pltpu.VMEM((2, 16, BLOCK, 768), F32),
            pltpu.VMEM((WAVES, 32, 768), F32),
            pltpu.VMEM((WAVES, 8, 32, 768), BF16),
            pltpu.VMEM((WAVES, 8, 32, 768), BF16),
            pltpu.VMEM((16, 8, 128), F32),
            pltpu.VMEM((8, 128), F32),
            dma((2,)), dma((LANES,)), dma((1,)),
            dma((1,)), dma((WAVES,)), dma((WAVES,)),
            dma((1,)), dma((WAVES,)),
            dma((1,)), dma((1,)),
            dma((4, LANES)), dma((4, LANES, 3)),
        ],
        compiler_params=pltpu.CompilerParams(
            collective_id=0, has_side_effects=True, vmem_limit_bytes=67043328
        ),
        name="ffn",
    )(tokens.reshape(WAVES, 32, 768), norm_gain, weight_in, weight_out)
    return out.reshape(128, 768)


def solution(mesh):
    in_specs = (P("col", "row"), P("row"), P("row", "col"), P("col", "row"))
    out_specs = P("col", "row")
    return jax.shard_map(
        per_device, mesh=mesh, in_specs=in_specs, out_specs=out_specs, check_vma=False
    )
```

```python
import functools

import jax
import jax.numpy as jnp
from jax import lax
from jax.experimental import pallas as pl
from jax.experimental.pallas import tpu as pltpu
from jax.sharding import PartitionSpec as P

D = 12288
EPSILON = 1e-05
MESH = pl.DeviceIdType.MESH
F32, BF16 = jnp.float32, jnp.bfloat16

WAVES = 4
LANES = 8
NARROW = 768
BLOCK = 16
TILE = 256


def gelu(v):
    return 0.5 * v * (1.0 + jnp.tanh(0.7978845608028654 * (v + 0.044715 * (v * v * v))))


def kernel(
    tokens_hbm, gain_hbm, w1_hbm, w2_hbm, out_ref,
    tokens_ref, gain_ref, w1, w2, raw, scaled, part, rs1, rs2, total, active, branch, own, out_send, out_recv, squares, inverse,
    in_sem, w1_sem, w2_sem, tok_ssem, tok_rsem, pair_rsem, out_ssem, out_rsem, sq_ssem, sq_rsem, ring_ssem, ring_rsem,
):
    row, col = lax.axis_index("row"), lax.axis_index("col")
    x, z = lax.rem(row, 4), lax.div(row, 4)

    def w1_copy(s):
        return pltpu.make_async_copy(w1_hbm.at[:, pl.ds(pl.multiple_of(s * NARROW, NARROW), NARROW)], w1.at[s], w1_sem.at[s])

    def w2_copy(s):
        return pltpu.make_async_copy(w2_hbm.at[pl.ds(pl.multiple_of(s * NARROW, NARROW), NARROW)], w2.at[s], w2_sem.at[0])

    inputs = (
        pltpu.make_async_copy(tokens_hbm, tokens_ref, in_sem.at[0]),
        pltpu.make_async_copy(gain_hbm, gain_ref, in_sem.at[1]),
    )
    inputs[0].start()
    barrier = pltpu.get_barrier_semaphore()
    for i in range(1, 8):
        pl.semaphore_signal(barrier, inc=1, device_id=(row, lax.rem(col + i, 8)), device_id_type=MESH)
    for i in range(1, 16):
        pl.semaphore_signal(barrier, inc=1, device_id=(lax.rem(row + i, 16), col), device_id_type=MESH)
    inputs[1].start()
    for s in range(LANES):
        w1_copy(s).start()

    inputs[0].wait()
    pl.semaphore_wait(barrier, 22)

    def landed(ref, sem):
        pltpu.make_async_copy(ref, ref, sem).wait()

    y, core = lax.div(col, 2), lax.rem(col, 2)
    partner = col + 1 - 2 * core

    def beside(n, c):
        return lax.rem(2 * (y + n) + c, 8)

    def source(w, g):
        late = lax.div(w, 2)
        two = lax.div(g, 2)
        odd = lax.rem(g, 2)
        early_c, late_c = beside(2 * w, two), beside(1 + 2 * two, odd)
        return early_c * (1 - late) + late_c * late, 4 * (odd * (1 - late) + (w - 2) * late)

    def tok_copy(w, n):
        blocks = pl.ds(0, 8) if w == 1 else pl.ds(4 * (w - 2), 4)
        return pltpu.make_async_remote_copy(
            src_ref=tokens_ref.at[blocks], dst_ref=raw.at[col, blocks],
            send_sem=tok_ssem.at[0], recv_sem=tok_rsem.at[w],
            device_id=(row, beside(n, core)), device_id_type=MESH,
        )

    def pair_copy(w, n):
        c = beside(n, core)
        blocks = pl.ds(0, 8) if w < 2 else pl.ds(4 * (w - 2), 4)
        return pltpu.make_async_remote_copy(
            src_ref=tokens_ref.at[blocks] if w == 0 else raw.at[c, blocks], dst_ref=raw.at[c, blocks],
            send_sem=tok_ssem.at[0], recv_sem=pair_rsem.at[w],
            device_id=(row, partner), device_id_type=MESH,
        )

    pair_copy(0, 0).start()
    tok_copy(1, 2).start()
    for w in (2, 3):
        for n in (1, 3):
            tok_copy(w, n).start()
    raw[col] = tokens_ref[...]

    def forward_tokens(w):
        landed(raw.at[0], tok_rsem.at[w])
        for n in (2,) if w == 1 else (1, 3):
            pair_copy(w, n).start()

    def wait_tokens(w):
        landed(raw.at[0], pair_rsem.at[w])

    def place(s):
        second = lax.rem(s, 2)
        step = 1 - 2 * lax.rem(lax.div(s, 2), 2)
        p = x * (1 - second) + z * second
        q = z * (1 - second) + x * second
        p_next, q_next = lax.rem(p + step + 4, 4), lax.rem(q + step + 4, 4)
        first_row = second * (p_next * 4 + q) + (1 - second) * (q * 4 + p_next)
        second_row = second * (p * 4 + q_next) + (1 - second) * (q_next * 4 + p)
        return p, q, step, first_row, second_row

    def ring_copy(kind, w, s, k, src, dst, target):
        return pltpu.make_async_remote_copy(
            src_ref=src, dst_ref=dst,
            send_sem=ring_ssem.at[kind, s], recv_sem=ring_rsem.at[kind if kind < 3 else 3 + lax.rem(w, 2), s, k],
            device_id=(target, col), device_id_type=MESH,
        )

    def around(v):
        return lax.rem(v + 8, 4)

    def rs1_copy(w, s, k, target):
        side = lax.rem(w, 2)
        return ring_copy(0, w, s, k, rs1.at[side, s, (k + 3) % 4], rs1.at[side, s, k], target)

    def rs2_copy(w, s, k, target):
        side = lax.rem(w, 2)
        return ring_copy(1, w, s, k, rs2.at[side, s, (k + 3) % 4], rs2.at[side, s, k], target)

    def ag2_copy(w, s, k, p, q, step, target):
        block = active.at[w, s, p * 4 + around(q - step * k)]
        return ring_copy(2, w, s, k, block, block, target)

    def ag1_copy(w, s, k, p, step, target):
        chunk = active.at[w, s, pl.ds(around(p - step * k) * 4, 4)]
        return ring_copy(3, w, s, k, chunk, chunk, target)

    def own_part(w, s):
        side = lax.rem(w, 2)
        for t in range(NARROW // TILE):
            cols = slice(t * TILE, (t + 1) * TILE)
            got = jnp.dot(scaled[w].reshape(256, 768), w1[s, :, cols], preferred_element_type=F32)
            part[side, s, :, :, cols] = got.reshape(16, BLOCK, TILE)

    def rs1_event(w, s, k):
        p, q, step, target, _ = place(s)
        j = around(p - step * (k + 1))
        side, slot = lax.rem(w, 2), (k + 3) % 4
        mine = part[side, s, pl.ds(j * 4, 4)]
        if k > 0:
            rs1_copy(w, s, k - 1, target).wait_recv()
            mine = mine + rs1[side, s, slot].astype(F32)
        rs1[side, s, slot] = mine.astype(BF16)
        if k > 0:
            rs1_copy(w, s, k - 1, target).wait_send()
        rs1_copy(w, s, k, target).start()

    def rs2_event(w, s, k):
        p, q, step, before, target = place(s)
        j = around(q - step * (k + 1))
        side, slot = lax.rem(w, 2), (k + 3) % 4
        if k == 0:
            rs1_copy(w, s, 2, before).wait_recv()
            total[s] = part[side, s, pl.ds(p * 4, 4)] + rs1[side, s, 2].astype(F32)
            rs1_copy(w, s, 2, before).wait_send()
            rs2[side, s, slot] = total[s, j].astype(BF16)
        else:
            rs2_copy(w, s, k - 1, target).wait_recv()
            rs2[side, s, slot] = (rs2[side, s, slot].astype(F32) + total[s, j]).astype(BF16)
            rs2_copy(w, s, k - 1, target).wait_send()
        rs2_copy(w, s, k, target).start()

    def ag2_event(w, s, k):
        p, q, step, _, target = place(s)
        if k == 0:
            rs2_copy(w, s, 2, target).wait_recv()
            b = p * 4 + q
            c, at = source(w, lax.div(b, 4))
            first = 16 * (at + lax.rem(b, 4))
            sub = lax.broadcasted_iota(jnp.int32, (8, 128), 0)
            line = jnp.sum(jnp.where(sub == c, inverse[...], 0.0), axis=0, keepdims=True)
            spot = lax.broadcasted_iota(jnp.int32, (BLOCK, 128), 1) == lax.broadcasted_iota(jnp.int32, (BLOCK, 128), 0) + first
            scale = jnp.sum(jnp.where(spot, jnp.broadcast_to(line, (BLOCK, 128)), 0.0), axis=1, keepdims=True)
            hidden = (rs2[lax.rem(w, 2), s, 2].astype(F32) + total[s, q]) * scale
            active[w, s, b] = gelu(hidden).astype(BF16)
            rs2_copy(w, s, 2, target).wait_send()
        else:
            ag2_copy(w, s, k - 1, p, q, step, target).wait_recv()
            ag2_copy(w, s, k - 1, p, q, step, target).wait_send()
        ag2_copy(w, s, k, p, q, step, target).start()

    def ag1_event(w, s, k):
        p, q, step, target, before = place(s)
        if k == 0:
            ag2_copy(w, s, 2, p, q, step, before).wait_recv()
            ag2_copy(w, s, 2, p, q, step, before).wait_send()

            @pl.when(w > 0)
            def _():
                ag1_copy(w, s, 2, p, step, target).wait_send()
        else:
            ag1_copy(w, s, k - 1, p, step, target).wait_recv()
            ag1_copy(w, s, k - 1, p, step, target).wait_send()
        ag1_copy(w, s, k, p, step, target).start()

    def out_copy(w, g, blocks):
        c, at = source(w, g)
        return pltpu.make_async_remote_copy(
            src_ref=out_send.at[w, pl.ds(4 * g, blocks)], dst_ref=out_recv.at[col, pl.ds(at, blocks)],
            send_sem=out_ssem.at[0], recv_sem=out_rsem.at[w],
            device_id=(row, c), device_id_type=MESH,
        )

    def add_chunks(w, s, ks):
        p, q, step, target, _ = place(s)
        side = lax.rem(w, 2)
        if 3 in ks:
            ag1_copy(w, s, 2, p, step, target).wait_recv()
        chunks = [pl.ds(around(p - step * k) * 4, 4) for k in ks]
        a = [active[w, s, chunk].reshape(64, NARROW) for chunk in chunks]
        a = a[0] if len(a) == 1 else jnp.concatenate(a, axis=0)
        for t in range(768 // TILE):
            cols = slice(t * TILE, (t + 1) * TILE)
            got = jnp.dot(a, w2[s, :, cols], preferred_element_type=F32)
            for n, chunk in enumerate(chunks):
                more = got[n * 64:(n + 1) * 64].reshape(4, BLOCK, TILE)
                branch[side, chunk, :, cols] = branch[side, chunk, :, cols] + more

    def send_branch(w):
        side = lax.rem(w, 2)

        @pl.when(w == 0)
        def _():
            g = 2 - 2 * core
            out_send[0, pl.ds(4 * g, 8)] = branch[side, pl.ds(4 * g, 8)].astype(BF16)
            out_copy(0, g, 8).start()
            own[...] = branch[side, pl.ds(8 * core, 8)]

        @pl.when(w == 1)
        def _():
            for g in (0, 2):
                out_send[1, pl.ds(4 * g, 8)] = branch[side, pl.ds(4 * g, 8)].astype(BF16)
                out_copy(1, g, 8).start()

        @pl.when(w > 1)
        def _():
            for g in (0, 2, 1, 3):
                out_send[w, pl.ds(4 * g, 4)] = branch[side, pl.ds(4 * g, 4)].astype(BF16)
                out_copy(w, g, 4).start()

    def deliver(h):
        blocks = pl.ds(4 * h, 4)
        rows = own[blocks] + tokens_ref[blocks].astype(F32)
        for n, c in ((0, 1 - core), (2, 0), (2, 1)):
            rows = rows + out_recv[beside(n, c), blocks].astype(F32)
        landed(out_recv.at[pl.ds(0, 2)], out_rsem.at[2 + h])
        for n, c in ((1, 0), (1, 1), (3, 0), (3, 1)):
            rows = rows + out_recv[beside(n, c), blocks].astype(F32)
        out_ref[blocks] = rows.astype(BF16)

    def sq_copy(i):
        return pltpu.make_async_remote_copy(
            src_ref=squares.at[row], dst_ref=squares.at[row],
            send_sem=sq_ssem.at[0], recv_sem=sq_rsem.at[0],
            device_id=(lax.rem(row + i, 16), col), device_id_type=MESH,
        )

    def square(c):
        v = raw[c].reshape(128, 768).astype(F32)
        v = v * v
        high = v.astype(BF16)
        low = (v - high.astype(F32)).astype(BF16)
        ones, dims = jnp.ones((8, 768), BF16), (((1,), (1,)), ((), ()))
        sums = lax.dot_general(ones, high, dims, preferred_element_type=F32)
        sums = sums + lax.dot_general(ones, low, dims, preferred_element_type=F32)
        squares[row, pl.ds(c, 1)] = sums[:1]

    def take_squares():
        landed(squares.at[pl.ds(0, 15)], sq_rsem.at[0])
        inverse[...] = lax.rsqrt(jnp.sum(squares[...], axis=0) / D + EPSILON)

    def scale_wave(w):
        def one(g, carry):
            c, at = source(w, g)
            v = raw[c, pl.ds(at, 4)].reshape(64, 768).astype(F32) * gain_ref[...].reshape(1, 768)
            scaled[w, pl.ds(4 * g, 4)] = v.astype(BF16).reshape(4, BLOCK, 768)
            return carry

        lax.fori_loop(0, 4, one, 0)

    inputs[1].wait()
    wait_tokens(0)
    scale_wave(0)

    def slot(t, carry):
        for k in range(3):
            if k == 0:
                @pl.when(t == 1)
                def _():
                    forward_tokens(2)
                    forward_tokens(3)

                @pl.when(t == 2)
                def _():
                    take_squares()

                @pl.when(t == 3)
                def _():
                    landed(w2, w2_sem.at[0])

                @pl.when((t >= 3) & (t < 7))
                def _():
                    branch[lax.rem(t + 1, 2)] = jnp.zeros((16, BLOCK, 768), F32)

            if k == 1:
                @pl.when((t > 0) & (t < 3))
                def _():
                    scale_wave(t + 1)

            if k == 2:
                @pl.when(t == 0)
                def _():
                    forward_tokens(1)

            def lane(s, carry, k=k):
                if k == 0:
                    @pl.when(t == 0)
                    def _():
                        w1_copy(s).wait()
                        own_part(0, s)

                    @pl.when((t == 1) & (s >= 4))
                    def _():
                        own_part(1, s)

                @pl.when((t >= 3) & (t < 7))
                def _():
                    ag1_event(t - 3, s, k)

                @pl.when((t >= 2) & (t < 6))
                def _():
                    ag2_event(t - 2, s, k)

                @pl.when((t >= 1) & (t < 5))
                def _():
                    rs2_event(t - 1, s, k)

                @pl.when(t < 4)
                def _():
                    rs1_event(t, s, k)

                if k == 0:
                    @pl.when((t == 1) & (s == 4))
                    def _():
                        wait_tokens(2)
                        wait_tokens(3)

                    @pl.when(t == 1)
                    def _():
                        near = lax.div(s, 4)
                        square((1 - near) * beside(2 * lax.div(s, 2), lax.rem(s, 2)) + near * beside(1 + 2 * lax.div(s - 4 * near, 2), lax.rem(s, 2)))

                if k > 0:
                    @pl.when((t > 0) & (t < 3) & (lax.rem(s, 2) == 1))
                    def _():
                        own_part(t + 1, 4 * (k - 1) + lax.div(s, 2))

                if k == 2:
                    @pl.when((t == 0) & (s == 3))
                    def _():
                        wait_tokens(1)
                        scale_wave(1)

                    @pl.when((t == 0) & (s >= 4))
                    def _():
                        own_part(1, s - 4)

                if k == 1:
                    @pl.when(t >= 4)
                    def _():
                        add_chunks(t - 4, s, (2, 3))

                if k == 2:
                    @pl.when(t >= 3)
                    def _():
                        add_chunks(t - 3, s, (0, 1))

                return carry

            lax.fori_loop(0, LANES, lane, 0)

            if k == 0:
                @pl.when(t == 0)
                def _():
                    for s in range(LANES):
                        w2_copy(s).start()

                @pl.when(t == 1)
                def _():
                    for i in range(1, 16):
                        sq_copy(i).start()

            if k == 1:
                @pl.when(t >= 4)
                def _():
                    send_branch(t - 4)

                @pl.when(t == 4)
                def _():
                    landed(raw.at[pl.ds(0, 7)], tok_ssem.at[0])
                    landed(squares.at[pl.ds(0, 15)], sq_ssem.at[0])

        return carry

    lax.fori_loop(0, 7, slot, 0)

    def last(s, carry):
        add_chunks(WAVES - 1, s, (2, 3))
        p, q, step, target, _ = place(s)
        ag1_copy(WAVES - 1, s, 2, p, step, target).wait_send()
        return carry

    lax.fori_loop(0, LANES, last, 0)
    send_branch(WAVES - 1)
    landed(out_recv.at[0], out_rsem.at[0])
    landed(out_recv.at[pl.ds(0, 2)], out_rsem.at[1])
    deliver(0)
    deliver(1)
    landed(out_send.at[:, pl.ds(0, 14)], out_ssem.at[0])


def per_device(tokens, norm_gain, weight_in, weight_out):
    vmem = pl.BlockSpec(memory_space=pltpu.VMEM)
    anywhere = pl.BlockSpec(memory_space=pl.ANY)
    dma = pltpu.SemaphoreType.DMA
    out = pl.pallas_call(
        kernel,
        out_shape=jax.ShapeDtypeStruct((8, BLOCK, 768), BF16),
        in_specs=[anywhere] * 4,
        out_specs=vmem,
        scratch_shapes=[
            pltpu.VMEM((8, BLOCK, 768), BF16),
            pltpu.VMEM((768,), F32),
            pltpu.VMEM((LANES, 768, NARROW), BF16),
            pltpu.VMEM((LANES, NARROW, 768), BF16),
            pltpu.VMEM((8, 8, BLOCK, 768), BF16),
            pltpu.VMEM((WAVES, 16, BLOCK, 768), BF16),
            pltpu.VMEM((2, LANES, 16, BLOCK, NARROW), F32),
            pltpu.VMEM((2, LANES, 4, 4, BLOCK, NARROW), BF16),
            pltpu.VMEM((2, LANES, 4, BLOCK, NARROW), BF16),
            pltpu.VMEM((LANES, 4, BLOCK, NARROW), F32),
            pltpu.VMEM((WAVES, LANES, 16, BLOCK, NARROW), BF16),
            pltpu.VMEM((2, 16, BLOCK, 768), F32),
            pltpu.VMEM((8, BLOCK, 768), F32),
            pltpu.VMEM((WAVES, 16, BLOCK, 768), BF16),
            pltpu.VMEM((8, 8, BLOCK, 768), BF16),
            pltpu.VMEM((16, 8, 128), F32),
            pltpu.VMEM((8, 128), F32),
            dma((2,)), dma((LANES,)), dma((1,)),
            dma((1,)), dma((WAVES,)), dma((WAVES,)),
            dma((1,)), dma((WAVES,)),
            dma((1,)), dma((1,)),
            dma((4, LANES)), dma((5, LANES, 3)),
        ],
        compiler_params=pltpu.CompilerParams(
            collective_id=0, has_side_effects=True, vmem_limit_bytes=67043328
        ),
        name="ffn",
    )(tokens.reshape(8, BLOCK, 768), norm_gain, weight_in, weight_out)
    return out.reshape(128, 768)


def solution(mesh):
    in_specs = (P("col", "row"), P("row"), P("row", "col"), P("col", "row"))
    out_specs = P("col", "row")
    return jax.shard_map(
        per_device, mesh=mesh, in_specs=in_specs, out_specs=out_specs, check_vma=False
    )
```

```python
import functools

import jax
import jax.numpy as jnp
from jax import lax
from jax.experimental import pallas as pl
from jax.experimental.pallas import tpu as pltpu
from jax.sharding import PartitionSpec as P

D = 12288
EPSILON = 1e-05
MESH = pl.DeviceIdType.MESH
F32, BF16 = jnp.float32, jnp.bfloat16

WAVES = 4
LANES = 8
NARROW = 768
BLOCK = 16
TILE = 256


def gelu(v):
    return 0.5 * v * (1.0 + jnp.tanh(0.7978845608028654 * (v + 0.044715 * (v * v * v))))


def kernel(
    tokens_hbm, gain_hbm, w1_hbm, w2_hbm, out_ref,
    tokens_ref, gain_ref, w1, w2, raw, scaled, part, rs1, rs2, total, active, branch, own, out_send, out_recv, squares, inverse,
    in_sem, w1_sem, w2_sem, tok_ssem, tok_rsem, pair_rsem, out_ssem, out_rsem, sq_ssem, sq_rsem, ring_ssem, ring_rsem,
):
    row, col = lax.axis_index("row"), lax.axis_index("col")
    x, z = lax.rem(row, 4), lax.div(row, 4)

    def w1_copy(s):
        return pltpu.make_async_copy(w1_hbm.at[:, pl.ds(pl.multiple_of(s * NARROW, NARROW), NARROW)], w1.at[s], w1_sem.at[s])

    def w2_copy(s):
        return pltpu.make_async_copy(w2_hbm.at[pl.ds(pl.multiple_of(s * NARROW, NARROW), NARROW)], w2.at[s], w2_sem.at[0])

    inputs = (
        pltpu.make_async_copy(tokens_hbm, tokens_ref, in_sem.at[0]),
        pltpu.make_async_copy(gain_hbm, gain_ref, in_sem.at[1]),
    )
    inputs[0].start()
    barrier = pltpu.get_barrier_semaphore()
    for i in range(1, 8):
        pl.semaphore_signal(barrier, inc=1, device_id=(row, lax.rem(col + i, 8)), device_id_type=MESH)
    for i in range(1, 4):
        pl.semaphore_signal(barrier, inc=1, device_id=(4 * z + lax.rem(x + i, 4), col), device_id_type=MESH)
        pl.semaphore_signal(barrier, inc=1, device_id=(4 * lax.rem(z + i, 4) + x, col), device_id_type=MESH)
    inputs[1].start()
    for s in range(4):
        w1_copy(s).start()

    inputs[0].wait()
    pl.semaphore_wait(barrier, 13)

    def landed(ref, sem):
        pltpu.make_async_copy(ref, ref, sem).wait()

    y, core = lax.div(col, 2), lax.rem(col, 2)
    partner = col + 1 - 2 * core

    def beside(n, c):
        return lax.rem(2 * (y + n) + c, 8)

    def source(w, g):
        late = lax.div(w, 2)
        two = lax.div(g, 2)
        odd = lax.rem(g, 2)
        early_c, late_c = beside(2 * w, two), beside(1 + 2 * two, odd)
        return early_c * (1 - late) + late_c * late, 4 * (odd * (1 - late) + (w - 2) * late)

    def tok_copy(w, n):
        blocks = pl.ds(0, 8) if w == 1 else pl.ds(4 * (w - 2), 4)
        return pltpu.make_async_remote_copy(
            src_ref=tokens_ref.at[blocks], dst_ref=raw.at[col, blocks],
            send_sem=tok_ssem.at[0], recv_sem=tok_rsem.at[w],
            device_id=(row, beside(n, core)), device_id_type=MESH,
        )

    def pair_copy(w, n):
        c = beside(n, core)
        blocks = pl.ds(0, 8) if w < 2 else pl.ds(4 * (w - 2), 4)
        return pltpu.make_async_remote_copy(
            src_ref=tokens_ref.at[blocks] if w == 0 else raw.at[c, blocks], dst_ref=raw.at[c, blocks],
            send_sem=tok_ssem.at[0], recv_sem=pair_rsem.at[w],
            device_id=(row, partner), device_id_type=MESH,
        )

    pair_copy(0, 0).start()
    raw[col] = tokens_ref[...]

    def forward_tokens(w):
        landed(raw.at[0], tok_rsem.at[w])
        for n in (2,) if w == 1 else (1, 3):
            pair_copy(w, n).start()

    def wait_tokens(w):
        landed(raw.at[0], pair_rsem.at[w])

    def place(s):
        second = lax.rem(s, 2)
        step = 1 - 2 * lax.rem(lax.div(s, 2), 2)
        p = x * (1 - second) + z * second
        q = z * (1 - second) + x * second
        p_next, q_next = lax.rem(p + step + 4, 4), lax.rem(q + step + 4, 4)
        first_row = second * (p_next * 4 + q) + (1 - second) * (q * 4 + p_next)
        second_row = second * (p * 4 + q_next) + (1 - second) * (q_next * 4 + p)
        return p, q, step, first_row, second_row

    def ring_copy(kind, w, s, k, src, dst, target):
        return pltpu.make_async_remote_copy(
            src_ref=src, dst_ref=dst,
            send_sem=ring_ssem.at[kind, s], recv_sem=ring_rsem.at[kind, s, k],
            device_id=(target, col), device_id_type=MESH,
        )

    def around(v):
        return lax.rem(v + 8, 4)

    def rs1_copy(w, s, k, target):
        side = lax.rem(w, 2)
        return ring_copy(0, w, s, k, rs1.at[side, s, (k + 3) % 4], rs1.at[side, s, k], target)

    def rs2_copy(w, s, k, target):
        side = lax.rem(w, 2)
        return ring_copy(1, w, s, k, rs2.at[side, s, (k + 3) % 4], rs2.at[side, s, k], target)

    def ag2_copy(w, s, k, p, q, step, target):
        block = active.at[w, s, p * 4 + around(q - step * k)]
        return ring_copy(2, w, s, k, block, block, target)

    def ag1_copy(w, s, k, p, step, target):
        chunk = active.at[w, s, pl.ds(around(p - step * k) * 4, 4)]
        return ring_copy(3, w, s, k, chunk, chunk, target)

    def own_part(w, s):
        side = lax.rem(w, 2)
        for t in range(NARROW // TILE):
            cols = slice(t * TILE, (t + 1) * TILE)
            got = jnp.dot(scaled[w].reshape(256, 768), w1[s, :, cols], preferred_element_type=F32)
            part[side, s, :, :, cols] = got.reshape(16, BLOCK, TILE)

    def rs1_event(w, s, k):
        p, q, step, target, _ = place(s)
        j = around(p - step * (k + 1))
        side, slot = lax.rem(w, 2), (k + 3) % 4
        mine = part[side, s, pl.ds(j * 4, 4)]
        if k > 0:
            rs1_copy(w, s, k - 1, target).wait_recv()
            mine = mine + rs1[side, s, slot].astype(F32)
        rs1[side, s, slot] = mine.astype(BF16)
        if k > 0:
            rs1_copy(w, s, k - 1, target).wait_send()
        rs1_copy(w, s, k, target).start()

    def rs2_event(w, s, k):
        p, q, step, before, target = place(s)
        j = around(q - step * (k + 1))
        side, slot = lax.rem(w, 2), (k + 3) % 4
        if k == 0:
            rs1_copy(w, s, 2, before).wait_recv()
            total[s] = part[side, s, pl.ds(p * 4, 4)] + rs1[side, s, 2].astype(F32)
            rs1_copy(w, s, 2, before).wait_send()
            rs2[side, s, slot] = total[s, j].astype(BF16)
        else:
            rs2_copy(w, s, k - 1, target).wait_recv()
            rs2[side, s, slot] = (rs2[side, s, slot].astype(F32) + total[s, j]).astype(BF16)
            rs2_copy(w, s, k - 1, target).wait_send()
        rs2_copy(w, s, k, target).start()

    def ag2_event(w, s, k):
        p, q, step, _, target = place(s)
        if k == 0:
            rs2_copy(w, s, 2, target).wait_recv()
            b = p * 4 + q
            c, at = source(w, lax.div(b, 4))
            first = 16 * (at + lax.rem(b, 4))
            sub = lax.broadcasted_iota(jnp.int32, (8, 128), 0)
            line = jnp.sum(jnp.where(sub == c, inverse[...], 0.0), axis=0, keepdims=True)
            spot = lax.broadcasted_iota(jnp.int32, (BLOCK, 128), 1) == lax.broadcasted_iota(jnp.int32, (BLOCK, 128), 0) + first
            scale = jnp.sum(jnp.where(spot, jnp.broadcast_to(line, (BLOCK, 128)), 0.0), axis=1, keepdims=True)
            hidden = (rs2[lax.rem(w, 2), s, 2].astype(F32) + total[s, q]) * scale
            active[w, s, b] = gelu(hidden).astype(BF16)
            rs2_copy(w, s, 2, target).wait_send()
        else:
            ag2_copy(w, s, k - 1, p, q, step, target).wait_recv()
            ag2_copy(w, s, k - 1, p, q, step, target).wait_send()
        ag2_copy(w, s, k, p, q, step, target).start()

    def ag1_event(w, s, k):
        p, q, step, target, before = place(s)
        if k == 0:
            ag2_copy(w, s, 2, p, q, step, before).wait_recv()
            ag2_copy(w, s, 2, p, q, step, before).wait_send()

            @pl.when(w > 0)
            def _():
                ag1_copy(w, s, 2, p, step, target).wait_send()
        else:
            ag1_copy(w, s, k - 1, p, step, target).wait_recv()
            ag1_copy(w, s, k - 1, p, step, target).wait_send()
        ag1_copy(w, s, k, p, step, target).start()

    def out_copy(w, g, blocks):
        c, at = source(w, g)
        return pltpu.make_async_remote_copy(
            src_ref=out_send.at[w, pl.ds(4 * g, blocks)], dst_ref=out_recv.at[col, pl.ds(at, blocks)],
            send_sem=out_ssem.at[0], recv_sem=out_rsem.at[w],
            device_id=(row, c), device_id_type=MESH,
        )

    def add_chunks(w, s, ks):
        p, q, step, target, _ = place(s)
        side = lax.rem(w, 2)
        chunks = [pl.ds(around(p - step * k) * 4, 4) for k in ks]
        a = [active[w, s, chunk].reshape(64, NARROW) for chunk in chunks]
        a = a[0] if len(a) == 1 else jnp.concatenate(a, axis=0)
        for t in range(768 // TILE):
            cols = slice(t * TILE, (t + 1) * TILE)
            got = jnp.dot(a, w2[s, :, cols], preferred_element_type=F32)
            for n, chunk in enumerate(chunks):
                more = got[n * 64:(n + 1) * 64].reshape(4, BLOCK, TILE)
                branch[side, chunk, :, cols] = branch[side, chunk, :, cols] + more

    def send_branch(w):
        side = lax.rem(w, 2)

        @pl.when(w == 0)
        def _():
            g = 2 - 2 * core
            out_send[0, pl.ds(4 * g, 8)] = branch[side, pl.ds(4 * g, 8)].astype(BF16)
            out_copy(0, g, 8).start()
            own[...] = branch[side, pl.ds(8 * core, 8)]

        @pl.when(w == 1)
        def _():
            for g in (0, 2):
                out_send[1, pl.ds(4 * g, 8)] = branch[side, pl.ds(4 * g, 8)].astype(BF16)
                out_copy(1, g, 8).start()

        @pl.when(w > 1)
        def _():
            for g in (0, 2, 1, 3):
                out_send[w, pl.ds(4 * g, 4)] = branch[side, pl.ds(4 * g, 4)].astype(BF16)
                out_copy(w, g, 4).start()

    def deliver(h):
        blocks = pl.ds(4 * h, 4)
        rows = own[blocks] + tokens_ref[blocks].astype(F32)
        for n, c in ((0, 1 - core), (2, 0), (2, 1)):
            rows = rows + out_recv[beside(n, c), blocks].astype(F32)
        landed(out_recv.at[pl.ds(0, 2)], out_rsem.at[2 + h])
        for n, c in ((1, 0), (1, 1), (3, 0), (3, 1)):
            rows = rows + out_recv[beside(n, c), blocks].astype(F32)
        out_ref[blocks] = rows.astype(BF16)

    def sq_copy(stage, i):
        place_here = z if stage else x
        peer = 4 * lax.rem(z + i, 4) + x if stage else 4 * z + lax.rem(x + i, 4)
        return pltpu.make_async_remote_copy(
            src_ref=squares.at[stage, place_here], dst_ref=squares.at[stage, place_here],
            send_sem=sq_ssem.at[0], recv_sem=sq_rsem.at[stage],
            device_id=(peer, col), device_id_type=MESH,
        )

    def square(c):
        v = raw[c].reshape(128, 768).astype(F32)
        v = v * v
        high = v.astype(BF16)
        low = (v - high.astype(F32)).astype(BF16)
        ones, dims = jnp.ones((8, 768), BF16), (((1,), (1,)), ((), ()))
        sums = lax.dot_general(ones, high, dims, preferred_element_type=F32)
        sums = sums + lax.dot_general(ones, low, dims, preferred_element_type=F32)
        squares[0, x, pl.ds(c, 1)] = sums[:1]

    def pass_squares():
        landed(squares.at[0, pl.ds(0, 3)], sq_rsem.at[0])
        squares[1, z] = jnp.sum(squares[0], axis=0)
        for i in range(1, 4):
            sq_copy(1, i).start()

    def take_squares():
        landed(squares.at[0, pl.ds(0, 3)], sq_rsem.at[1])
        inverse[...] = lax.rsqrt(jnp.sum(squares[1], axis=0) / D + EPSILON)

    def scale_wave(w):
        def one(g, carry):
            c, at = source(w, g)
            v = raw[c, pl.ds(at, 4)].reshape(64, 768).astype(F32) * gain_ref[...].reshape(1, 768)
            scaled[w, pl.ds(4 * g, 4)] = v.astype(BF16).reshape(4, BLOCK, 768)
            return carry

        lax.fori_loop(0, 4, one, 0)

    inputs[1].wait()
    wait_tokens(0)
    tok_copy(1, 2).start()
    for w in (2, 3):
        for n in (1, 3):
            tok_copy(w, n).start()
    scale_wave(0)
    for s in range(4, LANES):
        w1_copy(s).start()

    def slot(t, carry):
        for k in range(3):
            if k == 0:
                @pl.when(t == 1)
                def _():
                    forward_tokens(2)
                    forward_tokens(3)

                @pl.when(t == 2)
                def _():
                    take_squares()

                @pl.when(t == 3)
                def _():
                    landed(w2, w2_sem.at[0])

                @pl.when((t >= 3) & (t < 7))
                def _():
                    branch[lax.rem(t + 1, 2)] = jnp.zeros((16, BLOCK, 768), F32)

            if k == 1:
                @pl.when((t > 0) & (t < 3))
                def _():
                    scale_wave(t + 1)

            if k == 2:
                @pl.when(t == 0)
                def _():
                    forward_tokens(1)

            def lane(s, carry, k=k):
                if k == 0:
                    @pl.when(t == 0)
                    def _():
                        w1_copy(s).wait()
                        own_part(0, s)

                    @pl.when((t == 1) & (s >= 4))
                    def _():
                        own_part(1, s)

                @pl.when((t >= 3) & (t < 7))
                def _():
                    ag1_event(t - 3, s, k)

                @pl.when((t >= 2) & (t < 6))
                def _():
                    ag2_event(t - 2, s, k)

                @pl.when((t >= 1) & (t < 5))
                def _():
                    rs2_event(t - 1, s, k)

                @pl.when(t < 4)
                def _():
                    rs1_event(t, s, k)

                if k == 0:
                    @pl.when((t == 1) & (s == 4))
                    def _():
                        wait_tokens(2)
                        wait_tokens(3)

                    @pl.when(t == 1)
                    def _():
                        near = lax.div(s, 4)
                        square((1 - near) * beside(2 * lax.div(s, 2), lax.rem(s, 2)) + near * beside(1 + 2 * lax.div(s - 4 * near, 2), lax.rem(s, 2)))

                    @pl.when(t >= 4)
                    def _():
                        p, q, step, target, _ = place(s)
                        ag1_copy(t - 4, s, 2, p, step, target).wait_recv()

                if k > 0:
                    @pl.when((t > 0) & (t < 3) & (lax.rem(s, 2) == 1))
                    def _():
                        own_part(t + 1, 4 * (k - 1) + lax.div(s, 2))

                if k == 2:
                    @pl.when((t == 0) & (s == 3))
                    def _():
                        wait_tokens(1)
                        scale_wave(1)

                    @pl.when((t == 0) & (s >= 4))
                    def _():
                        own_part(1, s - 4)

                if k == 1:
                    @pl.when(t >= 4)
                    def _():
                        add_chunks(t - 4, s, (2, 3))

                if k == 2:
                    @pl.when(t >= 3)
                    def _():
                        add_chunks(t - 3, s, (0, 1))

                return carry

            lax.fori_loop(0, LANES, lane, 0)

            if k == 0:
                @pl.when(t == 0)
                def _():
                    for s in range(LANES):
                        w2_copy(s).start()

                @pl.when(t == 1)
                def _():
                    for i in range(1, 4):
                        sq_copy(0, i).start()

            if k == 1:
                @pl.when(t == 1)
                def _():
                    pass_squares()

                @pl.when(t >= 4)
                def _():
                    send_branch(t - 4)

                @pl.when(t == 4)
                def _():
                    landed(raw.at[pl.ds(0, 7)], tok_ssem.at[0])
                    landed(squares.at[:, pl.ds(0, 3)], sq_ssem.at[0])

        return carry

    lax.fori_loop(0, 7, slot, 0)

    def last(s, carry):
        p, q, step, target, _ = place(s)
        ag1_copy(WAVES - 1, s, 2, p, step, target).wait_recv()
        add_chunks(WAVES - 1, s, (2, 3))
        ag1_copy(WAVES - 1, s, 2, p, step, target).wait_send()
        return carry

    lax.fori_loop(0, LANES, last, 0)
    send_branch(WAVES - 1)
    landed(out_recv.at[0], out_rsem.at[0])
    landed(out_recv.at[pl.ds(0, 2)], out_rsem.at[1])
    deliver(0)
    deliver(1)
    landed(out_send.at[:, pl.ds(0, 14)], out_ssem.at[0])


def per_device(tokens, norm_gain, weight_in, weight_out):
    vmem = pl.BlockSpec(memory_space=pltpu.VMEM)
    anywhere = pl.BlockSpec(memory_space=pl.ANY)
    dma = pltpu.SemaphoreType.DMA
    out = pl.pallas_call(
        kernel,
        out_shape=jax.ShapeDtypeStruct((8, BLOCK, 768), BF16),
        in_specs=[anywhere] * 4,
        out_specs=vmem,
        scratch_shapes=[
            pltpu.VMEM((8, BLOCK, 768), BF16),
            pltpu.VMEM((768,), F32),
            pltpu.VMEM((LANES, 768, NARROW), BF16),
            pltpu.VMEM((LANES, NARROW, 768), BF16),
            pltpu.VMEM((8, 8, BLOCK, 768), BF16),
            pltpu.VMEM((WAVES, 16, BLOCK, 768), BF16),
            pltpu.VMEM((2, LANES, 16, BLOCK, NARROW), F32),
            pltpu.VMEM((2, LANES, 4, 4, BLOCK, NARROW), BF16),
            pltpu.VMEM((2, LANES, 4, BLOCK, NARROW), BF16),
            pltpu.VMEM((LANES, 4, BLOCK, NARROW), F32),
            pltpu.VMEM((WAVES, LANES, 16, BLOCK, NARROW), BF16),
            pltpu.VMEM((2, 16, BLOCK, 768), F32),
            pltpu.VMEM((8, BLOCK, 768), F32),
            pltpu.VMEM((WAVES, 16, BLOCK, 768), BF16),
            pltpu.VMEM((8, 8, BLOCK, 768), BF16),
            pltpu.VMEM((2, 4, 8, 128), F32),
            pltpu.VMEM((8, 128), F32),
            dma((2,)), dma((LANES,)), dma((1,)),
            dma((1,)), dma((WAVES,)), dma((WAVES,)),
            dma((1,)), dma((WAVES,)),
            dma((1,)), dma((2,)),
            dma((4, LANES)), dma((4, LANES, 3)),
        ],
        compiler_params=pltpu.CompilerParams(
            collective_id=0, has_side_effects=True, vmem_limit_bytes=67043328
        ),
        name="ffn",
    )(tokens.reshape(8, BLOCK, 768), norm_gain, weight_in, weight_out)
    return out.reshape(128, 768)


def solution(mesh):
    in_specs = (P("col", "row"), P("row"), P("row", "col"), P("col", "row"))
    out_specs = P("col", "row")
    return jax.shard_map(
        per_device, mesh=mesh, in_specs=in_specs, out_specs=out_specs, check_vma=False
    )
```

```python
import functools

import jax
import jax.numpy as jnp
from jax import lax
from jax.experimental import pallas as pl
from jax.experimental.pallas import tpu as pltpu
from jax.sharding import PartitionSpec as P

D = 12288
EPSILON = 1e-05
MESH = pl.DeviceIdType.MESH
F32, BF16 = jnp.float32, jnp.bfloat16

WAVES = 4
LANES = 8
NARROW = 768
BLOCK = 16
TILE = 256


def gelu(v):
    return 0.5 * v * (1.0 + jnp.tanh(0.7978845608028654 * (v + 0.044715 * (v * v * v))))


def kernel(
    tokens_hbm, gain_hbm, w1_hbm, w2_hbm, out_ref,
    tokens_ref, gain_ref, w1, w2, raw, scaled, part, rs1, rs2, total, active, branch, own, out_send, out_recv, squares, inverse,
    in_sem, w1_sem, w2_sem, tok_ssem, tok_rsem, pair_rsem, out_ssem, out_rsem, sq_ssem, sq_rsem, ring_ssem, ring_rsem,
):
    row, col = lax.axis_index("row"), lax.axis_index("col")
    x, z = lax.rem(row, 4), lax.div(row, 4)

    def w1_copy(s):
        return pltpu.make_async_copy(w1_hbm.at[:, pl.ds(pl.multiple_of(s * NARROW, NARROW), NARROW)], w1.at[s], w1_sem.at[s])

    def w2_copy(s):
        return pltpu.make_async_copy(w2_hbm.at[pl.ds(pl.multiple_of(s * NARROW, NARROW), NARROW)], w2.at[s], w2_sem.at[0])

    inputs = (
        pltpu.make_async_copy(tokens_hbm, tokens_ref, in_sem.at[0]),
        pltpu.make_async_copy(gain_hbm, gain_ref, in_sem.at[1]),
    )
    inputs[0].start()
    barrier = pltpu.get_barrier_semaphore()
    for i in range(1, 8):
        pl.semaphore_signal(barrier, inc=1, device_id=(row, lax.rem(col + i, 8)), device_id_type=MESH)
    for i in range(1, 4):
        pl.semaphore_signal(barrier, inc=1, device_id=(4 * z + lax.rem(x + i, 4), col), device_id_type=MESH)
        pl.semaphore_signal(barrier, inc=1, device_id=(4 * lax.rem(z + i, 4) + x, col), device_id_type=MESH)
    inputs[1].start()
    for s in range(4):
        w1_copy(s).start()

    inputs[0].wait()
    pl.semaphore_wait(barrier, 13)

    def landed(ref, sem):
        pltpu.make_async_copy(ref, ref, sem).wait()

    y, core = lax.div(col, 2), lax.rem(col, 2)
    partner = col + 1 - 2 * core

    def beside(n, c):
        return lax.rem(2 * (y + n) + c, 8)

    def source(w, g):
        late = lax.div(w, 2)
        two = lax.div(g, 2)
        odd = lax.rem(g, 2)
        early_c, late_c = beside(2 * w, two), beside(1 + 2 * two, odd)
        return early_c * (1 - late) + late_c * late, 4 * (odd * (1 - late) + (w - 2) * late)

    def tok_copy(w, n):
        blocks = pl.ds(0, 8) if w == 1 else pl.ds(4 * (w - 2), 4)
        return pltpu.make_async_remote_copy(
            src_ref=tokens_ref.at[blocks], dst_ref=raw.at[col, blocks],
            send_sem=tok_ssem.at[0], recv_sem=tok_rsem.at[w],
            device_id=(row, beside(n, core)), device_id_type=MESH,
        )

    def pair_copy(w, n):
        c = beside(n, core)
        blocks = pl.ds(0, 8) if w < 2 else pl.ds(4 * (w - 2), 4)
        return pltpu.make_async_remote_copy(
            src_ref=tokens_ref.at[blocks] if w == 0 else raw.at[c, blocks], dst_ref=raw.at[c, blocks],
            send_sem=tok_ssem.at[0], recv_sem=pair_rsem.at[w],
            device_id=(row, partner), device_id_type=MESH,
        )

    pair_copy(0, 0).start()
    raw[col] = tokens_ref[...]

    def forward_tokens(w):
        landed(raw.at[0], tok_rsem.at[w])
        for n in (2,) if w == 1 else (1, 3):
            pair_copy(w, n).start()

    def wait_tokens(w):
        landed(raw.at[0], pair_rsem.at[w])

    def place(s):
        second = lax.rem(s, 2)
        step = 1 - 2 * lax.rem(lax.div(s, 2), 2)
        p = x * (1 - second) + z * second
        q = z * (1 - second) + x * second
        p_next, q_next = lax.rem(p + step + 4, 4), lax.rem(q + step + 4, 4)
        first_row = second * (p_next * 4 + q) + (1 - second) * (q * 4 + p_next)
        second_row = second * (p * 4 + q_next) + (1 - second) * (q_next * 4 + p)
        return p, q, step, first_row, second_row

    def ring_copy(kind, w, s, k, src, dst, target):
        return pltpu.make_async_remote_copy(
            src_ref=src, dst_ref=dst,
            send_sem=ring_ssem.at[kind, s], recv_sem=ring_rsem.at[kind, s, k],
            device_id=(target, col), device_id_type=MESH,
        )

    def around(v):
        return lax.rem(v + 8, 4)

    def rs1_copy(w, s, k, target):
        side = lax.rem(w, 2)
        return ring_copy(0, w, s, k, rs1.at[side, s, (k + 3) % 4], rs1.at[side, s, k], target)

    def rs2_copy(w, s, k, target):
        side = lax.rem(w, 2)
        return ring_copy(1, w, s, k, rs2.at[side, s, (k + 3) % 4], rs2.at[side, s, k], target)

    def ag2_copy(w, s, k, p, q, step, target):
        block = active.at[w, s, p * 4 + around(q - step * k)]
        return ring_copy(2, w, s, k, block, block, target)

    def ag1_copy(w, s, k, p, step, target):
        chunk = active.at[w, s, pl.ds(around(p - step * k) * 4, 4)]
        return ring_copy(3, w, s, k, chunk, chunk, target)

    def own_part(w, s):
        side = lax.rem(w, 2)
        for t in range(NARROW // TILE):
            cols = slice(t * TILE, (t + 1) * TILE)
            got = jnp.dot(scaled[w].reshape(256, 768), w1[s, :, cols], preferred_element_type=F32)
            part[side, s, :, :, cols] = got.reshape(16, BLOCK, TILE)

    def rs1_event(w, s, k):
        p, q, step, target, _ = place(s)
        j = around(p - step * (k + 1))
        side, slot = lax.rem(w, 2), (k + 3) % 4
        mine = part[side, s, pl.ds(j * 4, 4)]
        if k > 0:
            rs1_copy(w, s, k - 1, target).wait_recv()
            mine = mine + rs1[side, s, slot].astype(F32)
        rs1[side, s, slot] = mine.astype(BF16)
        if k > 0:
            rs1_copy(w, s, k - 1, target).wait_send()
        rs1_copy(w, s, k, target).start()

    def rs2_event(w, s, k):
        p, q, step, before, target = place(s)
        j = around(q - step * (k + 1))
        side, slot = lax.rem(w, 2), (k + 3) % 4
        if k == 0:
            rs1_copy(w, s, 2, before).wait_recv()
            total[s] = part[side, s, pl.ds(p * 4, 4)] + rs1[side, s, 2].astype(F32)
            rs1_copy(w, s, 2, before).wait_send()
            rs2[side, s, slot] = total[s, j].astype(BF16)
        else:
            rs2_copy(w, s, k - 1, target).wait_recv()
            rs2[side, s, slot] = (rs2[side, s, slot].astype(F32) + total[s, j]).astype(BF16)
            rs2_copy(w, s, k - 1, target).wait_send()
        rs2_copy(w, s, k, target).start()

    def ag2_event(w, s, k):
        p, q, step, _, target = place(s)
        if k == 0:
            rs2_copy(w, s, 2, target).wait_recv()
            b = p * 4 + q
            c, at = source(w, lax.div(b, 4))
            first = 16 * (at + lax.rem(b, 4))
            sub = lax.broadcasted_iota(jnp.int32, (8, 128), 0)
            line = jnp.sum(jnp.where(sub == c, inverse[...], 0.0), axis=0, keepdims=True)
            spot = lax.broadcasted_iota(jnp.int32, (BLOCK, 128), 1) == lax.broadcasted_iota(jnp.int32, (BLOCK, 128), 0) + first
            scale = jnp.sum(jnp.where(spot, jnp.broadcast_to(line, (BLOCK, 128)), 0.0), axis=1, keepdims=True)
            hidden = (rs2[lax.rem(w, 2), s, 2].astype(F32) + total[s, q]) * scale
            active[w, s, b] = gelu(hidden).astype(BF16)
            rs2_copy(w, s, 2, target).wait_send()
        else:
            ag2_copy(w, s, k - 1, p, q, step, target).wait_recv()
            ag2_copy(w, s, k - 1, p, q, step, target).wait_send()
        ag2_copy(w, s, k, p, q, step, target).start()

    def ag1_event(w, s, k):
        p, q, step, target, before = place(s)
        if k == 0:
            ag2_copy(w, s, 2, p, q, step, before).wait_recv()
            ag2_copy(w, s, 2, p, q, step, before).wait_send()

            @pl.when(w > 0)
            def _():
                ag1_copy(w, s, 2, p, step, target).wait_send()
        else:
            ag1_copy(w, s, k - 1, p, step, target).wait_recv()
            ag1_copy(w, s, k - 1, p, step, target).wait_send()
        ag1_copy(w, s, k, p, step, target).start()

    def out_copy(w, g, blocks):
        c, at = source(w, g)
        return pltpu.make_async_remote_copy(
            src_ref=out_send.at[w, pl.ds(4 * g, blocks)], dst_ref=out_recv.at[col, pl.ds(at, blocks)],
            send_sem=out_ssem.at[0], recv_sem=out_rsem.at[w],
            device_id=(row, c), device_id_type=MESH,
        )

    def add_chunks(w, s, ks):
        p, q, step, target, _ = place(s)
        side = lax.rem(w, 2)
        chunks = [pl.ds(around(p - step * k) * 4, 4) for k in ks]
        a = [active[w, s, chunk].reshape(64, NARROW) for chunk in chunks]
        a = a[0] if len(a) == 1 else jnp.concatenate(a, axis=0)
        for t in range(768 // TILE):
            cols = slice(t * TILE, (t + 1) * TILE)
            got = jnp.dot(a, w2[s, :, cols], preferred_element_type=F32)
            for n, chunk in enumerate(chunks):
                more = got[n * 64:(n + 1) * 64].reshape(4, BLOCK, TILE)
                branch[side, chunk, :, cols] = branch[side, chunk, :, cols] + more

    def send_branch(w):
        side = lax.rem(w, 2)

        @pl.when(w == 0)
        def _():
            g = 2 - 2 * core
            out_send[0, pl.ds(4 * g, 8)] = branch[side, pl.ds(4 * g, 8)].astype(BF16)
            out_copy(0, g, 8).start()
            own[...] = branch[side, pl.ds(8 * core, 8)]

        @pl.when(w == 1)
        def _():
            for g in (0, 2):
                out_send[1, pl.ds(4 * g, 8)] = branch[side, pl.ds(4 * g, 8)].astype(BF16)
                out_copy(1, g, 8).start()

        @pl.when(w > 1)
        def _():
            for g in (0, 2, 1, 3):
                out_send[w, pl.ds(4 * g, 4)] = branch[side, pl.ds(4 * g, 4)].astype(BF16)
                out_copy(w, g, 4).start()

    def deliver(h):
        blocks = pl.ds(4 * h, 4)
        rows = own[blocks] + tokens_ref[blocks].astype(F32)
        for n, c in ((0, 1 - core), (2, 0), (2, 1)):
            rows = rows + out_recv[beside(n, c), blocks].astype(F32)
        landed(out_recv.at[pl.ds(0, 2)], out_rsem.at[2 + h])
        for n, c in ((1, 0), (1, 1), (3, 0), (3, 1)):
            rows = rows + out_recv[beside(n, c), blocks].astype(F32)
        out_ref[blocks] = rows.astype(BF16)

    def sq_copy(stage, i):
        place_here = z if stage else x
        peer = 4 * lax.rem(z + i, 4) + x if stage else 4 * z + lax.rem(x + i, 4)
        return pltpu.make_async_remote_copy(
            src_ref=squares.at[stage, place_here], dst_ref=squares.at[stage, place_here],
            send_sem=sq_ssem.at[0], recv_sem=sq_rsem.at[stage],
            device_id=(peer, col), device_id_type=MESH,
        )

    def square(c):
        v = raw[c].reshape(128, 768).astype(F32)
        v = v * v
        high = v.astype(BF16)
        low = (v - high.astype(F32)).astype(BF16)
        ones, dims = jnp.ones((8, 768), BF16), (((1,), (1,)), ((), ()))
        sums = lax.dot_general(ones, high, dims, preferred_element_type=F32)
        sums = sums + lax.dot_general(ones, low, dims, preferred_element_type=F32)
        squares[0, x, pl.ds(c, 1)] = sums[:1]

    def pass_squares():
        landed(squares.at[0, pl.ds(0, 3)], sq_rsem.at[0])
        squares[1, z] = jnp.sum(squares[0], axis=0)
        for i in range(1, 4):
            sq_copy(1, i).start()

    def take_squares():
        landed(squares.at[0, pl.ds(0, 3)], sq_rsem.at[1])
        inverse[...] = lax.rsqrt(jnp.sum(squares[1], axis=0) / D + EPSILON)

    def scale_wave(w):
        def one(g, carry):
            c, at = source(w, g)
            v = raw[c, pl.ds(at, 4)].reshape(64, 768).astype(F32) * gain_ref[...].reshape(1, 768)
            scaled[w, pl.ds(4 * g, 4)] = v.astype(BF16).reshape(4, BLOCK, 768)
            return carry

        lax.fori_loop(0, 4, one, 0)

    inputs[1].wait()
    wait_tokens(0)
    tok_copy(1, 2).start()
    for w in (2, 3):
        for n in (1, 3):
            tok_copy(w, n).start()
    scale_wave(0)
    for s in range(4, LANES):
        w1_copy(s).start()

    def in_turn(s):
        return s + (1 - core) * (2 - 4 * lax.rem(lax.div(s, 2), 2))

    def slot(t, carry):
        for k in range(3):
            if k == 0:
                @pl.when(t == 1)
                def _():
                    forward_tokens(2)
                    forward_tokens(3)

                @pl.when(t == 2)
                def _():
                    take_squares()

                @pl.when(t == 3)
                def _():
                    landed(w2, w2_sem.at[0])

                @pl.when((t >= 3) & (t < 7))
                def _():
                    branch[lax.rem(t + 1, 2)] = jnp.zeros((16, BLOCK, 768), F32)

            if k == 1:
                @pl.when((t > 0) & (t < 3))
                def _():
                    scale_wave(t + 1)

            if k == 2:
                @pl.when(t == 0)
                def _():
                    forward_tokens(1)

            def lane(s, carry, k=k):
                e = in_turn(s)
                if k == 0:
                    @pl.when(t == 0)
                    def _():
                        w1_copy(e).wait()
                        own_part(0, e)

                    @pl.when((t == 1) & (s >= 4))
                    def _():
                        own_part(1, e)

                @pl.when((t >= 3) & (t < 7))
                def _():
                    ag1_event(t - 3, e, k)

                @pl.when((t >= 2) & (t < 6))
                def _():
                    ag2_event(t - 2, e, k)

                @pl.when((t >= 1) & (t < 5))
                def _():
                    rs2_event(t - 1, e, k)

                @pl.when(t < 4)
                def _():
                    rs1_event(t, e, k)

                if k == 0:
                    @pl.when((t == 1) & (s == 4))
                    def _():
                        wait_tokens(2)
                        wait_tokens(3)

                    @pl.when(t == 1)
                    def _():
                        near = lax.div(s, 4)
                        square((1 - near) * beside(2 * lax.div(s, 2), lax.rem(s, 2)) + near * beside(1 + 2 * lax.div(s - 4 * near, 2), lax.rem(s, 2)))

                    @pl.when(t >= 4)
                    def _():
                        p, q, step, target, _ = place(e)
                        ag1_copy(t - 4, e, 2, p, step, target).wait_recv()

                if k > 0:
                    @pl.when((t > 0) & (t < 3) & (lax.rem(s, 2) == 1))
                    def _():
                        own_part(t + 1, 4 * (k - 1) + lax.div(s, 2))

                if k == 2:
                    @pl.when((t == 0) & (s == 3))
                    def _():
                        wait_tokens(1)
                        scale_wave(1)

                    @pl.when((t == 0) & (s >= 4))
                    def _():
                        own_part(1, s - 4)

                if k == 1:
                    @pl.when(t >= 4)
                    def _():
                        add_chunks(t - 4, e, (2, 3))

                if k == 2:
                    @pl.when(t >= 3)
                    def _():
                        add_chunks(t - 3, e, (0, 1))

                return carry

            lax.fori_loop(0, LANES, lane, 0)

            if k == 0:
                @pl.when(t == 0)
                def _():
                    for s in range(LANES):
                        w2_copy(s).start()

                @pl.when(t == 1)
                def _():
                    for i in range(1, 4):
                        sq_copy(0, i).start()

            if k == 1:
                @pl.when(t == 1)
                def _():
                    pass_squares()

                @pl.when(t >= 4)
                def _():
                    send_branch(t - 4)

                @pl.when(t == 4)
                def _():
                    landed(raw.at[pl.ds(0, 7)], tok_ssem.at[0])
                    landed(squares.at[:, pl.ds(0, 3)], sq_ssem.at[0])

        return carry

    lax.fori_loop(0, 7, slot, 0)

    def last(s, carry):
        s = in_turn(s)
        p, q, step, target, _ = place(s)
        ag1_copy(WAVES - 1, s, 2, p, step, target).wait_recv()
        add_chunks(WAVES - 1, s, (2, 3))
        ag1_copy(WAVES - 1, s, 2, p, step, target).wait_send()
        return carry

    lax.fori_loop(0, LANES, last, 0)
    send_branch(WAVES - 1)
    landed(out_recv.at[0], out_rsem.at[0])
    landed(out_recv.at[pl.ds(0, 2)], out_rsem.at[1])
    deliver(0)
    deliver(1)
    landed(out_send.at[:, pl.ds(0, 14)], out_ssem.at[0])


def per_device(tokens, norm_gain, weight_in, weight_out):
    vmem = pl.BlockSpec(memory_space=pltpu.VMEM)
    anywhere = pl.BlockSpec(memory_space=pl.ANY)
    dma = pltpu.SemaphoreType.DMA
    out = pl.pallas_call(
        kernel,
        out_shape=jax.ShapeDtypeStruct((8, BLOCK, 768), BF16),
        in_specs=[anywhere] * 4,
        out_specs=vmem,
        scratch_shapes=[
            pltpu.VMEM((8, BLOCK, 768), BF16),
            pltpu.VMEM((768,), F32),
            pltpu.VMEM((LANES, 768, NARROW), BF16),
            pltpu.VMEM((LANES, NARROW, 768), BF16),
            pltpu.VMEM((8, 8, BLOCK, 768), BF16),
            pltpu.VMEM((WAVES, 16, BLOCK, 768), BF16),
            pltpu.VMEM((2, LANES, 16, BLOCK, NARROW), F32),
            pltpu.VMEM((2, LANES, 4, 4, BLOCK, NARROW), BF16),
            pltpu.VMEM((2, LANES, 4, BLOCK, NARROW), BF16),
            pltpu.VMEM((LANES, 4, BLOCK, NARROW), F32),
            pltpu.VMEM((WAVES, LANES, 16, BLOCK, NARROW), BF16),
            pltpu.VMEM((2, 16, BLOCK, 768), F32),
            pltpu.VMEM((8, BLOCK, 768), F32),
            pltpu.VMEM((WAVES, 16, BLOCK, 768), BF16),
            pltpu.VMEM((8, 8, BLOCK, 768), BF16),
            pltpu.VMEM((2, 4, 8, 128), F32),
            pltpu.VMEM((8, 128), F32),
            dma((2,)), dma((LANES,)), dma((1,)),
            dma((1,)), dma((WAVES,)), dma((WAVES,)),
            dma((1,)), dma((WAVES,)),
            dma((1,)), dma((2,)),
            dma((4, LANES)), dma((4, LANES, 3)),
        ],
        compiler_params=pltpu.CompilerParams(
            collective_id=0, has_side_effects=True, vmem_limit_bytes=67043328
        ),
        name="ffn",
    )(tokens.reshape(8, BLOCK, 768), norm_gain, weight_in, weight_out)
    return out.reshape(128, 768)


def solution(mesh):
    in_specs = (P("col", "row"), P("row"), P("row", "col"), P("col", "row"))
    out_specs = P("col", "row")
    return jax.shard_map(
        per_device, mesh=mesh, in_specs=in_specs, out_specs=out_specs, check_vma=False
    )
```
